32 devices in a mesh: blk: 8 (over z, x), grp: 4 (over y, core).
Axes of the slice: x: 2, y: 2, z: 4, core: 2. Of those that a mesh axis runs over, the one named last changes fastest.
Arguments:
- coil_pos: float32 [3, 1280], P(None, ('blk', 'grp')), may hold values from -1 to 1
- coil_radius: float32 [1280], P(('blk', 'grp')), may hold values from 0.02 to 0.08
- coil_current: bfloat16 [64, 1280], P(None, ('blk', 'grp')), may hold values from -0.3125 to 0.3125
- blank_pos: float32 [3, 4096], P(None, ('blk', 'grp')), may hold values from -1 to 1
- blank_rule: int32 [4096], P(('blk', 'grp')), may hold values from 0 to 7
- blank_cond: float32 [4096], P(('blk', 'grp')), may hold values from 0.3 to 3
- quad_offset: float32 [3, 8, 2], replicated, may hold values from -0.1 to 0.1
- quad_weight: float32 [8, 2], replicated, may hold values from 0.3 to 0.7
Outputs:
- blank_current: bfloat16 [64, 4096], P(None, ('blk', 'grp'))
- coil_reaction: float32 [64, 1280], P(None, ('blk', 'grp'))
The draws below stay inside these ranges and needn't reach their ends.
All inputs are finite; a program needn't handle non-finite values.
Results may differ from the reference program's by a relative error of at most 0.0066.
Values may be sent and summed in bfloat16 or wider, within the bound.
A program may use at most 64 MiB of HBM per device.

```python
import math
import jax
import jax.numpy as jnp
from jax import lax

COIL_DEV = 40
SAMPLES = 64
QUAD = 2
RULES = 8
COILS = 1280
BLANKS = 4096


def plant(result, rng, least, top_value):
    spot = [jax.random.randint(jax.random.fold_in(rng, axis), (), 0, length) for axis, length in enumerate(result.shape)]
    widest = result.shape.index(max(result.shape))
    next_to = spot[:widest] + [(spot[widest] + 1) % result.shape[widest]] + spot[widest + 1:]
    return result.at[tuple(spot)].set(least).at[tuple(next_to)].set(top_value)


def block_scale(key, shape, pieces, low, high):
    loudness = 1.0
    for axis_at, shards_of in pieces:
        steps = jax.random.uniform(jax.random.fold_in(jax.random.fold_in(key, 6), axis_at), (shards_of,), jnp.float32, low / len(pieces), high / len(pieces))
        loudness = loudness * jnp.repeat(jnp.exp(steps), shape[axis_at] // shards_of).reshape((-1,) + (1,) * (len(shape) - 1 - axis_at))
    return loudness


def centred(rng, extent, spread, limit, shards=(), kind=jnp.bfloat16):
    result = jax.random.normal(rng, extent, jnp.float32) * spread
    if len(shards) > 0:
        result = block_scale(rng, extent, shards, -0.22, 0.18) * result
    return jnp.clip(result, min=-limit, max=limit).astype(kind)


def setup_inputs(seed: int = 0) -> dict:
    key_list = jax.random.split(jax.random.key(seed), 9)
    return {
        "coil_pos": jnp.clip(jax.random.uniform(key_list[0], (3, COILS), jnp.float32, -1.0, 1.0) * block_scale(key_list[0], (3, COILS), ((1, 32),), -0.4, 0.0), -1.0, 1.0),
        "coil_radius": jnp.clip(jnp.exp(math.log(0.08) - 1.3862944 * jax.random.uniform(key_list[1], (COILS,), jnp.float32) ** block_scale(key_list[1], (COILS,), ((0, 32),), -0.2, 0.2)), 0.02, 0.08),
        "coil_current": centred(key_list[2], (SAMPLES, COILS), (0.7 / COILS ** 0.5), 0.3125, ((1, 32),)),
        "blank_pos": jnp.clip(jax.random.uniform(key_list[3], (3, BLANKS), jnp.float32, -1.0, 1.0) * block_scale(key_list[3], (3, BLANKS), ((1, 32),), -0.4, 0.0), -1.0, 1.0),
        "blank_rule": plant(jax.random.randint(key_list[4], (BLANKS,), 0, RULES), jax.random.fold_in(key_list[4], 1), 0, RULES - 1).astype(jnp.int32),
        "blank_cond": jnp.clip(jnp.exp(math.log(3.0) - 2.3025851 * jax.random.uniform(key_list[5], (BLANKS,), jnp.float32) ** block_scale(key_list[5], (BLANKS,), ((0, 32),), -0.2, 0.2)), 0.3, 3.0),
        "quad_offset": jnp.clip(jax.random.uniform(key_list[6], (3, RULES, QUAD), jnp.float32, -0.1, 0.1), -0.1, 0.1),
        "quad_weight": jnp.clip(jax.random.uniform(key_list[7], (RULES, QUAD), jnp.float32, 0.3, 0.7), 0.3, 0.7),
    }


def blank_geometry(blank_pos, blank_rule, quad_offset, quad_weight):
    rules = quad_weight.shape[0]
    points = quad_weight.shape[1]
    onehot = (blank_rule[None, :] == jnp.arange(rules, dtype=jnp.int32)[:, None]).astype(jnp.float32)
    table_rows = []
    base_rows = []
    zeros_row = jnp.zeros_like(blank_pos[0])
    for point in range(points):
        table_rows += [quad_offset[0, :, point], quad_offset[1, :, point], quad_offset[2, :, point], quad_weight[:, point]]
        base_rows += [blank_pos[0], blank_pos[1], blank_pos[2], zeros_row]
    table = jnp.stack(table_rows, 0)
    base = jnp.stack(base_rows, 0)
    return base + jnp.dot(table, onehot, precision=lax.Precision.HIGHEST)

def kernel_block(coil_geometry, geometry):
    points = geometry.shape[0] // 4
    running = jnp.zeros((coil_geometry.shape[1], geometry.shape[1]), jnp.float32)
    for point in range(points):
        delta_x = coil_geometry[0][:, None] - geometry[4 * point][None, :]
        delta_y = coil_geometry[1][:, None] - geometry[4 * point + 1][None, :]
        delta_z = coil_geometry[2][:, None] - geometry[4 * point + 2][None, :]
        squared = delta_x * delta_x + delta_y * delta_y + delta_z * delta_z + coil_geometry[3][:, None]
        running = running + geometry[4 * point + 3][None, :] * lax.rsqrt(squared)
    return running

def reference(coil_pos, coil_radius, coil_current, blank_pos, blank_rule, blank_cond, quad_offset, quad_weight):
    coil_geometry = jnp.concatenate([coil_pos, (coil_radius * coil_radius)[None, :]], 0)
    geometry = blank_geometry(blank_pos, blank_rule, quad_offset, quad_weight)
    groups = COILS // COIL_DEV
    grouped_geometry = coil_geometry.reshape(4, groups, COIL_DEV).transpose(1, 0, 2)
    grouped_current = coil_current.reshape(SAMPLES, groups, COIL_DEV).transpose(1, 0, 2)

    def first_pass(running, inputs):
        group_geometry, group_current = inputs
        kernel_tile = kernel_block(group_geometry, geometry).astype(jnp.bfloat16)
        return (running + jnp.dot(group_current, kernel_tile, preferred_element_type=jnp.float32), None)
    induced, _ = lax.scan(first_pass, jnp.zeros((SAMPLES, BLANKS), jnp.float32), (grouped_geometry, grouped_current))
    blank_current = induced.astype(jnp.bfloat16)
    weighted = (blank_cond[None, :] * blank_current.astype(jnp.float32)).astype(jnp.bfloat16)

    def second_pass(carried, group_geometry):
        kernel_tile = kernel_block(group_geometry, geometry).astype(jnp.bfloat16)
        product = lax.dot_general(weighted, kernel_tile, (((1,), (1,)), ((), ())), preferred_element_type=jnp.float32)
        return (carried, product)
    _, portions = lax.scan(second_pass, jnp.zeros((), jnp.float32), grouped_geometry)
    coil_reaction = portions.transpose(1, 0, 2).reshape(SAMPLES, COILS) * (2.0 / BLANKS)
    return (blank_current, coil_reaction)
```

```python
import functools

import jax
import jax.numpy as jnp
from jax import lax
from jax.experimental import pallas as pl
from jax.experimental.pallas import tpu as pltpu
from jax.sharding import PartitionSpec as P

MESH = pl.DeviceIdType.MESH
LANES = 128


def split3(value):
    first = value.astype(jnp.bfloat16).astype(jnp.float32)
    rest = value - first
    second = rest.astype(jnp.bfloat16).astype(jnp.float32)
    third = (rest - second).astype(jnp.bfloat16).astype(jnp.float32)
    return first, second, third


def kernel(
    blks, pairs, offsets, scale,
    cpos, crad, ccur, bpos, brule, bcond, qoff, qw,
    blank_out, react_out,
    held, geo, gmat, kern, part, outgo, income, flip,
    send_sem, recv_sem, geo_send, geo_recv, part_send, part_recv, rsend_sem, rrecv_sem,
):
    samples, coils = ccur.shape
    blanks = bpos.shape[1]
    rules, points = qw.shape
    n = blks * pairs
    stride = held.shape[0] // n
    blk = lax.axis_index("blk")
    grp = lax.axis_index("grp")
    core = lax.rem(grp, 2)
    pair = lax.div(grp, 2)
    sibling = (blk, pair * 2 + 1 - core)

    def peer(index, sign):
        db, dp = offsets[index]
        if sign < 0:
            db, dp = (blks - db) % blks, (pairs - dp) % pairs
        return (lax.rem(blk + db, blks), lax.rem(pair + dp, pairs) * 2 + core)

    barrier = pltpu.get_barrier_semaphore()
    for k in range(n - 1, 0, -1):
        pl.semaphore_signal(barrier, inc=1, device_id=peer(k, 1), device_id_type=MESH)
    pl.semaphore_signal(barrier, inc=1, device_id=sibling, device_id_type=MESH)

    flip[...] = jnp.zeros_like(flip)
    flip[0:samples, 0:coils] = ccur[...].astype(jnp.float32)
    radius = crad[...].reshape(1, coils)
    xyz = [cpos[c : c + 1, :] for c in range(3)]
    fixed = xyz[0] * xyz[0] + xyz[1] * xyz[1] + xyz[2] * xyz[2] + radius * radius
    ones = jnp.ones((1, coils), jnp.float32)
    rows = []
    for c in range(3):
        a, b, d = split3(xyz[c])
        rows += [a, a, a, b, b, d]
    rows += list(split3(fixed)) + [ones, ones, ones]
    for f, row in enumerate(rows):
        flip[samples + f : samples + f + 1, 0:coils] = row
    flip[samples + 18 : samples + 19, coils:LANES] = jnp.ones((1, LANES - coils), jnp.float32)
    turned = jnp.transpose(flip[...])[0:stride].astype(jnp.bfloat16)
    held[0:stride, :] = turned
    if stride > coils:
        for k in range(1, n):
            held[k * stride + coils : (k + 1) * stride, :] = turned[coils:stride]

    onehot = (
        brule[...].reshape(1, blanks) == lax.broadcasted_iota(jnp.int32, (rules, blanks), 0)
    ).astype(jnp.float32)
    geo[0] = jnp.zeros(geo.shape[1:], jnp.float32)
    for q in range(points):
        for c in range(3):
            geo[0, 4 * q + c : 4 * q + c + 1, :] = bpos[c : c + 1, :] + jnp.sum(
                onehot * qoff[c][:, q : q + 1], axis=0, keepdims=True
            )
        geo[0, 4 * q + 3 : 4 * q + 4, :] = jnp.sum(
            onehot * qw[:, q : q + 1], axis=0, keepdims=True
        )
    geo[0, 4 * points : 4 * points + 1, :] = bcond[...].reshape(1, blanks)

    pl.semaphore_wait(barrier, n)

    copies = [None] * n
    for k in range(n - 1, 0, -1):
        copies[k] = pltpu.make_async_remote_copy(
            src_ref=held.at[pl.ds(0, coils)],
            dst_ref=held.at[pl.ds(k * stride, coils)],
            send_sem=send_sem.at[k],
            recv_sem=recv_sem.at[k],
            device_id=peer(k, 1),
            device_id_type=MESH,
        )
        copies[k].start()
    geo_copy = pltpu.make_async_remote_copy(
        src_ref=geo.at[0], dst_ref=geo.at[1], send_sem=geo_send, recv_sem=geo_recv,
        device_id=sibling, device_id_type=MESH,
    )
    geo_copy.start()
    geo_copy.wait()

    def wide(row):
        return jnp.concatenate([geo[0, row : row + 1, :], geo[1, row : row + 1, :]], axis=1)

    width = 2 * blanks
    gmat[...] = jnp.zeros_like(gmat)
    feature_block = []
    for q in range(points):
        pos = [wide(4 * q + c) for c in range(3)]
        square = pos[0] * pos[0] + pos[1] * pos[1] + pos[2] * pos[2]
        one = jnp.ones((1, width), jnp.float32)
        rows = []
        for c in range(3):
            a, b, d = (-2.0 * v for v in split3(pos[c]))
            rows += [a, b, d, a, b, a]
        rows += [one, one, one] + list(split3(square))
        feature_block.append(jnp.concatenate(rows, axis=0))
    gmat[samples : samples + len(rows), :] = jnp.concatenate(feature_block, axis=1).astype(
        jnp.bfloat16
    )
    weights = [wide(4 * q + 3) for q in range(points)]
    cond = wide(4 * points)

    group = 4 if n % 4 == 0 else 1
    total = jnp.zeros((LANES, width), jnp.float32)
    for first in range(0, n, group):
        for k in range(first, first + group):
            if k > 0:
                copies[k].wait_recv()
        block = held[first * stride : (first + group) * stride, :]
        squared = jnp.dot(block, gmat[...], preferred_element_type=jnp.float32)
        tile = weights[0] * lax.rsqrt(squared[:, 0:width])
        for q in range(1, points):
            tile = tile + weights[q] * lax.rsqrt(squared[:, q * width : (q + 1) * width])
        tile = tile.astype(jnp.bfloat16)
        kern[first * stride : (first + group) * stride, :] = tile
        total = total + lax.dot_general(
            block, tile, (((0,), (0,)), ((), ())), preferred_element_type=jnp.float32
        )
    part[0] = total[0:samples]
    part_copy = pltpu.make_async_remote_copy(
        src_ref=part.at[0], dst_ref=part.at[1], send_sem=part_send, recv_sem=part_recv,
        device_id=sibling, device_id_type=MESH,
    )
    part_copy.start()
    part_copy.wait_recv()
    other = jnp.concatenate([part[1, :, blanks:width], part[1, :, 0:blanks]], axis=1)
    induced = (total[0:samples] + other).astype(jnp.bfloat16)
    blank_out[...] = induced[:, 0:blanks]
    weighted = (cond * induced.astype(jnp.float32)).astype(jnp.bfloat16)
    weighted = jnp.concatenate(
        [weighted, jnp.zeros((LANES - samples, width), jnp.bfloat16)], axis=0
    )

    returns = [None] * n
    own = None
    for first in range(n - group, -1, -group):
        product = lax.dot_general(
            kern[first * stride : (first + group) * stride, :],
            weighted,
            (((1,), (1,)), ((), ())),
            preferred_element_type=jnp.float32,
        )
        if first == 0:
            own = product[0:coils]
        outgo[first * stride : (first + group) * stride, :] = product.astype(jnp.bfloat16)
        for k in range(first + group - 1, first - 1, -1):
            if k > 0:
                returns[k] = pltpu.make_async_remote_copy(
                    src_ref=outgo.at[pl.ds(k * stride, coils)],
                    dst_ref=income.at[pl.ds(k * stride, coils)],
                    send_sem=rsend_sem.at[k],
                    recv_sem=rrecv_sem.at[k],
                    device_id=peer(k, -1),
                    device_id_type=MESH,
                )
                returns[k].start()

    flip[...] = jnp.zeros_like(flip)
    for k in range(1, n):
        copies[k].wait_send()
    part_copy.wait_send()
    for k in range(1, n):
        returns[k].wait_recv()
        own = own + income[k * stride : k * stride + coils, :].astype(jnp.float32)
    flip[0:coils, :] = own * scale
    react_out[...] = jnp.transpose(flip[...])[0:samples, 0:coils]
    for k in range(1, n):
        returns[k].wait_send()


def per_device(
    blks, grps,
    coil_pos, coil_radius, coil_current, blank_pos, blank_rule, blank_cond, quad_offset, quad_weight,
):
    pairs = grps // 2
    n = blks * pairs
    samples, coils = coil_current.shape
    blanks = blank_pos.shape[1]
    points = quad_weight.shape[1]
    stride = -(-coils // 16) * 16
    offsets = sorted(
        ((b, p) for b in range(blks) for p in range(pairs)),
        key=lambda o: min(o[0], blks - o[0]) + min(o[1], pairs - o[1]),
    )
    scale = 2.0 / (blanks * blks * grps)
    vmem = pl.BlockSpec(memory_space=pltpu.VMEM)
    return pl.pallas_call(
        functools.partial(kernel, blks, pairs, tuple(offsets), scale),
        out_shape=(
            jax.ShapeDtypeStruct((samples, blanks), jnp.bfloat16),
            jax.ShapeDtypeStruct((samples, coils), jnp.float32),
        ),
        in_specs=[vmem] * 8,
        out_specs=(vmem, vmem),
        scratch_shapes=[
            pltpu.VMEM((n * stride, LANES), jnp.bfloat16),
            pltpu.VMEM((2, -(-(4 * points + 1) // 8) * 8, blanks), jnp.float32),
            pltpu.VMEM((LANES, points * 2 * blanks), jnp.bfloat16),
            pltpu.VMEM((n * stride, 2 * blanks), jnp.bfloat16),
            pltpu.VMEM((2, samples, 2 * blanks), jnp.float32),
            pltpu.VMEM((n * stride, LANES), jnp.bfloat16),
            pltpu.VMEM((n * stride, LANES), jnp.bfloat16),
            pltpu.VMEM((LANES, LANES), jnp.float32),
            pltpu.SemaphoreType.DMA((n,)),
            pltpu.SemaphoreType.DMA((n,)),
            pltpu.SemaphoreType.DMA,
            pltpu.SemaphoreType.DMA,
            pltpu.SemaphoreType.DMA,
            pltpu.SemaphoreType.DMA,
            pltpu.SemaphoreType.DMA((n,)),
            pltpu.SemaphoreType.DMA((n,)),
        ],
        compiler_params=pltpu.CompilerParams(collective_id=0, has_side_effects=True),
    )(
        coil_pos, coil_radius, coil_current, blank_pos, blank_rule, blank_cond,
        quad_offset, quad_weight,
    )


def solution(mesh):
    split = ("blk", "grp")
    in_specs = (
        P(None, split), P(split), P(None, split), P(None, split), P(split), P(split), P(), P(),
    )
    return jax.shard_map(
        functools.partial(per_device, mesh.shape["blk"], mesh.shape["grp"]),
        mesh=mesh,
        in_specs=in_specs,
        out_specs=(P(None, split), P(None, split)),
        check_vma=False,
    )
```
